32 devices in a mesh: pair: 8 (over z, y), occ: 4 (over x, core).
Axes of the slice: x: 2, y: 2, z: 4, core: 2. Of those that a mesh axis runs over, the one named last changes fastest.
Arguments:
- amplitudes: float32 [64, 128, 128], P('pair'), may hold values from -4 to 4
- exchange_ints: float32 [64, 128, 128], P('pair'), may hold values from -6 to 6
- pno_energy: float32 [64, 128], P('pair'), may hold values from 0.3 to 3
- pair_shift: float32 [64], P('pair'), may hold values from 0.5 to 2
- coefficients: bfloat16 [64, 512, 128], P('pair'), may hold values from -0.5 to 0.5
- domain_tiles: int32 [64, 4], P('pair'), may hold values from 0 to 3, each once within a row
- couple_owner: int32 [4, 64, 2, 1], P('occ', 'pair'), may hold values from 0 to 7; in each aligned block of 16 rows (0 to 15, 16 to 31, ..., all dimensions but the last counted through in order) at most 3 rows name the same one
- couple_index: int32 [4, 64, 2], P('occ', 'pair'), may hold values from 0 to 7
- couple_weight: float32 [4, 64, 2], P('occ', 'pair'), may hold values from -0.5 to 0.5
Outputs:
- final_amplitudes: float32 [64, 128, 128], P('pair')
- final_residual: float32 [64, 128, 128], P('pair')
The draws below stay inside these ranges and needn't reach their ends.
Inputs may be any that keep to these rules, and one draw needn't show every extreme that they name: `couple_owner`: among the couplings held by one device (one block of 16 entries), no owner is named more than 3 times. `domain_tiles`: the tiles of one pair's domain are distinct.
All inputs are finite; a program needn't handle non-finite values.
Results may differ from the reference program's by a relative error of at most 0.0003.
Values may be sent and summed in bfloat16 or wider, within the bound.
No kernel may reach another device: no remote copies, remote signals or barrier semaphores. Data moves between devices by JAX's collectives and lax.ppermute only.
A program may use at most 128 MiB of HBM per device.

```python
import math
import jax
import jax.numpy as jnp
import numpy as np
from jax import lax

NPNO = 128
TILE = 128
DOM_TILES = 4
PAIR_DEV = 8
ITERS = 2
DOMAIN = 512
PAIRS = 64
NCOUP_DEV = 2
CAP = 3
N_PAIR = 8
N_OCC = 4


def place_ends(values, own_key, smallest, largest):
    shape = values.shape
    spot = [jax.random.randint(jax.random.fold_in(own_key, axis), (), 0, shape[axis]) for axis in range(len(shape))]
    values = values.at[tuple(spot)].set(smallest)
    longest = shape.index(max(shape))
    spot[longest] = (spot[longest] + 1) % shape[longest]
    return values.at[tuple(spot)].set(largest)


def steps_of(rng, extent, cuts, smallest, high):
    def one(position, shards_of):
        draws = jax.random.uniform(jax.random.fold_in(jax.random.fold_in(rng, 6), position), (shards_of,), jnp.float32, smallest / len(cuts), high / len(cuts))
        return jnp.repeat(jnp.exp(draws), extent[position] // shards_of).reshape((-1,) + (1,) * (len(extent) - position - 1))

    loudness = one(*cuts[0])
    for cut in cuts[1:]:
        loudness = loudness * one(*cut)
    return loudness


def assign_block(stream_key, own, number, rows, number_of, top, limit, lean):
    sequence = jax.random.permutation(stream_key, number_of)
    crowded, ordinary = load_shares(number_of, rows * top, limit, lean, True), load_shares(number_of, rows * top, limit, lean, False)
    places = jnp.arange(number_of)

    def named(lengths, turn):
        used = int((lengths > 0).sum())
        fixed = max(1, used // 4)
        shifted = fixed + (places - fixed + turn * (used - fixed)) % max(1, number_of - fixed)
        return jnp.zeros((number_of,), jnp.int32).at[sequence[jnp.where(places < fixed, places, shifted)]].set(jnp.asarray(lengths, jnp.int32))

    lengths = jnp.where(number % 4 == 0, named(crowded, number // 4), named(ordinary, number - number // 4 - 1))
    mixed = jax.random.permutation(jax.random.fold_in(own, 3), number_of)
    giver, taker = mixed[0:number_of // 2 * 2:2], mixed[1:number_of // 2 * 2:2]
    margin = jnp.minimum(lengths[giver] - 1, limit - lengths[taker]) // 2
    margin = jnp.where((giver == sequence[0]) | (taker == sequence[0]) | (lengths[taker] == 0), 0, jnp.maximum(margin, 0))
    shifted = jax.random.randint(jax.random.fold_in(own, 4), (number_of // 2,), 0, 1 << 20) % (margin + 1)
    lengths = lengths.at[giver].add(-shifted).at[taker].add(shifted)
    labels = jnp.searchsorted(jnp.cumsum(lengths), jnp.arange(rows * top), side="right").astype(jnp.int32)
    listing = labels.reshape(top, rows).T
    listing = listing[jax.random.permutation(jax.random.fold_in(own, 1), rows)]
    turn = jax.random.randint(jax.random.fold_in(own, 2), (rows, 1), 0, top)
    return jnp.take_along_axis(listing, (jnp.arange(top)[None, :] + turn) % top, axis=1)


def load_shares(count, total, most, slope, full):
    loads = [(1 << 20) // math.isqrt(rank ** slope) + 1 for rank in range(1, count + 1)]
    largest = most if full else min(most, max(-(-total // count), total * loads[0] // sum(loads)))
    least = 1 if total - largest >= count - 1 else 0
    holding, spare = [largest] + [least] * (count - 1), total - largest - least * (count - 1)
    while spare > 0:
        free = [i for i in range(1, count) if holding[i] < largest] or [i for i in range(1, count) if holding[i] < most]
        whole, left = sum([loads[i] for i in free]), spare
        for i in free:
            extra = min(most - holding[i], max(1, left * loads[i] // whole), spare)
            holding[i] = holding[i] + extra
            spare = spare - extra
    return np.array(holding)


def bell_draw(key, dims, width, reach, cuts=(), kind=jnp.bfloat16):
    gain = steps_of(key, dims, cuts, -0.22, 0.18) if cuts else 1.0
    values = jax.random.normal(key, dims, jnp.float32) * width * gain
    return jnp.minimum(jnp.maximum(values, -reach), reach).astype(kind)


def setup_inputs(seed: int = 0) -> dict:
    arg_keys = jax.random.split(jax.random.key(seed), 10)
    amplitudes = bell_draw(arg_keys[0], (PAIRS, NPNO, NPNO), 0.3, 4.0, ((0, 8),), jnp.float32)
    exchange_ints = bell_draw(arg_keys[1], (PAIRS, NPNO, NPNO), 1.0, 6.0, ((0, 8),), jnp.float32)
    pno_energy = jnp.clip(jnp.exp(math.log(3.0) - 2.3025851 * jax.random.uniform(arg_keys[2], (PAIRS, NPNO), jnp.float32) ** steps_of(arg_keys[2], (PAIRS, NPNO), ((0, 8),), -0.2, 0.2)), 0.3, 3.0)
    pair_shift = jnp.clip(0.5 + 1.5 * jax.random.uniform(arg_keys[3], (PAIRS,), jnp.float32) ** steps_of(arg_keys[3], (PAIRS,), ((0, 8),), -0.2, 0.2), 0.5, 2.0)
    coefficients = bell_draw(arg_keys[4], (PAIRS, DOMAIN, NPNO), TILE ** -0.5, 0.5, ((0, 8),))
    domain_tiles = jax.vmap(lambda own: jax.random.permutation(own, DOM_TILES))(jax.random.split(arg_keys[5], PAIRS)).reshape((PAIRS, DOM_TILES)).astype(jnp.int32)
    couple_owner_keys = jax.random.split(jax.random.fold_in(arg_keys[6], 1), N_OCC * PAIRS * NCOUP_DEV // (PAIR_DEV * NCOUP_DEV))
    couple_owner_turns = jax.random.permutation(jax.random.fold_in(arg_keys[6], 3), N_OCC * PAIRS * NCOUP_DEV // (PAIR_DEV * NCOUP_DEV))
    couple_owner = jax.vmap(lambda own, number: assign_block(jax.random.fold_in(arg_keys[6], 2), own, number, PAIR_DEV * NCOUP_DEV, N_PAIR, 1, CAP, 2))(couple_owner_keys, couple_owner_turns).reshape((N_OCC, PAIRS, NCOUP_DEV, 1))
    couple_index = place_ends(jax.random.randint(arg_keys[7], (N_OCC, PAIRS, NCOUP_DEV), 0, PAIR_DEV), jax.random.fold_in(arg_keys[7], 1), 0, PAIR_DEV - 1).astype(jnp.int32)
    couple_weight = bell_draw(arg_keys[8], (N_OCC, PAIRS, NCOUP_DEV), 0.08, 0.5, ((0, 4), (1, 8)), jnp.float32)
    return dict(amplitudes=amplitudes, exchange_ints=exchange_ints, pno_energy=pno_energy, pair_shift=pair_shift, coefficients=coefficients, domain_tiles=domain_tiles, couple_owner=couple_owner, couple_index=couple_index, couple_weight=couple_weight)


HIGHEST = lax.Precision.HIGHEST


def moved_onto(own_tiles, partner_tiles, partner_coef):
    total_count = partner_coef.shape[0]
    tile_match = (own_tiles[None, :, None] == partner_tiles[:, None, :]).astype(jnp.float32)
    tile_blocks = partner_coef.astype(jnp.float32).reshape(total_count, DOM_TILES, TILE * NPNO)
    moved_tiles = jnp.einsum('cab,cbx->cax', tile_match, tile_blocks, precision=HIGHEST)
    return moved_tiles.reshape(total_count, DOM_TILES * TILE, NPNO)


def reference(amplitudes, exchange_ints, pno_energy, pair_shift, coefficients, domain_tiles, couple_owner, couple_index, couple_weight):
    partner = (couple_owner[..., 0] * PAIR_DEV + couple_index).astype(jnp.int32)
    partner = jnp.transpose(partner, (1, 0, 2)).reshape(PAIRS, N_OCC * NCOUP_DEV)
    weights = jnp.transpose(couple_weight, (1, 0, 2)).reshape(PAIRS, N_OCC * NCOUP_DEV)
    denominator = pno_energy[:, :, None] + pno_energy[:, None, :] + pair_shift[:, None, None]

    def coupled(current):
        def one_pair(pair_index):
            partner_rows = partner[pair_index]
            own_coef = coefficients[pair_index].astype(jnp.float32)
            moved_tiles = moved_onto(domain_tiles[pair_index], domain_tiles[partner_rows], coefficients[partner_rows])
            intersection = jnp.einsum('fa,cfb->cab', own_coef, moved_tiles, precision=HIGHEST)
            inner_prod = jnp.einsum('cab,cbd->cad', intersection, current[partner_rows], precision=HIGHEST)
            outer_prod = jnp.einsum('cad,ced->cae', inner_prod, intersection, precision=HIGHEST)
            return jnp.einsum('c,cae->ae', weights[pair_index], outer_prod, precision=HIGHEST)
        return lax.map(one_pair, jnp.arange(PAIRS, dtype=jnp.int32))

    current = amplitudes
    residual = amplitudes
    for iteration in range(ITERS):
        residual = exchange_ints + denominator * current - coupled(current)
        current = current - residual / denominator
    return current, residual
```

```python
import functools

import jax
import jax.numpy as jnp
import numpy as np
from jax import lax
from jax.experimental import pallas as pl
from jax.experimental.pallas import tpu as pltpu
from jax.sharding import PartitionSpec as P

ITERS = 2
UNROLL = 2
F32 = jnp.float32
BF16 = jnp.bfloat16
VMEM = pltpu.VMEM
SMEM = pltpu.SMEM


def ring_order(mesh):
    count = mesh.shape["pair"]
    try:
        spots = [tuple(d.coords)[1:3] for d in mesh.devices[:, 0]]
    except Exception:
        return list(range(count))
    ys = sorted({s[0] for s in spots})
    zs = sorted({s[1] for s in spots})
    where = {s: i for i, s in enumerate(spots)}
    if len(where) != count or len(ys) * len(zs) != count:
        return list(range(count))
    if len(zs) % 2 == 0:
        rows, cols, at = zs, ys, lambda r, c: (c, r)
    else:
        rows, cols, at = ys, zs, lambda r, c: (r, c)
    if len(rows) % 2 or len(cols) == 1:
        return list(range(count))
    walk = [at(rows[0], cols[0])]
    for i, r in enumerate(rows):
        inner = cols[1:] if i % 2 == 0 else cols[:0:-1]
        walk += [at(r, c) for c in inner]
    walk += [at(r, cols[0]) for r in rows[:0:-1]]
    return [where[s] for s in walk]


def ring_table(order):
    count = len(order)
    table = np.zeros((count, count), np.int32)
    for spot, device in enumerate(order):
        held = [device]
        for step in range(1, count // 2 + 1):
            held.append(order[(spot - step) % count])
            if len(held) < count:
                held.append(order[(spot + step) % count])
        table[device] = held[:count]
    return table


def ring_gather(order, own):
    count = len(order)
    right = [(order[i], order[(i + 1) % count]) for i in range(count)]
    left = [(b, a) for a, b in right]
    held = [own]
    ahead = behind = own
    for step in range(1, count // 2 + 1):
        ahead = lax.ppermute(ahead, "pair", right)
        held.append(ahead)
        if len(held) < count:
            behind = lax.ppermute(behind, "pair", left)
            held.append(behind)
    return held


def prep_kernel(per, tiles_ref, coef_ref, amp_ref, coef_out, amp_out, sem):
    first = lax.axis_index("occ") * per
    tiles = tiles_ref.shape[1]
    copies = [pltpu.make_async_copy(amp_ref.at[pl.ds(first, per)], amp_out, sem.at[per * tiles])]
    for i in range(per):
        for b in range(tiles):
            region = tiles_ref[first + i, b]
            copies.append(
                pltpu.make_async_copy(
                    coef_ref.at[first + i, b], coef_out.at[i, region], sem.at[i * tiles + b]
                )
            )
    for c in copies:
        c.start()
    for c in copies:
        c.wait()


def turn_kernel(tiles_ref, coef_ref, out_ref):
    pairs, tiles, size, width = coef_ref.shape
    for p in range(pairs):
        for b in range(tiles):
            at = pl.multiple_of(tiles_ref[p, b] * size, size)
            out_ref[p, :, pl.ds(at, size)] = coef_ref[p, b].T


def split(value):
    high = value.astype(BF16)
    low = (value - high.astype(F32)).astype(BF16)
    return high, low


def overlap_kernel(couples, table_ref, slot_ref, weight_ref, turned_ref, *refs):
    count = table_ref.shape[1]
    shards = refs[:count]
    s_out, pair_out, slot_out, weight_out, used_out, held, sem = refs[count:]
    me = lax.axis_index("pair")
    per = shards[0].shape[0]
    copies = []
    for k in range(count):
        at = table_ref[me, k] * per
        copies.append(pltpu.make_async_copy(shards[k], held.at[pl.ds(at, per)], sem.at[k]))
    for c in copies:
        c.start()

    def listing(j, used):
        slot = slot_ref[j]
        pair_out[used] = j // couples
        slot_out[used] = slot
        weight_out[used] = weight_ref[j]
        return used + jnp.where(slot >= 0, 1, 0)

    used = lax.fori_loop(0, slot_ref.shape[0], listing, 0)
    for k in range(UNROLL):
        pair_out[used + k] = 0
        slot_out[used + k] = 0
        weight_out[used + k] = 0.0
    used_out[0] = used
    for c in copies:
        c.wait()

    def step(g, carry):
        for k in range(UNROLL):
            i = g * UNROLL + k
            value = jnp.dot(turned_ref[pair_out[i]], held[slot_out[i]], preferred_element_type=F32)
            high, low = split(value)
            width = high.shape[1]
            s_out[i, :, :width] = high
            s_out[i, :, width:] = low
        return carry

    lax.fori_loop(0, (used + UNROLL - 1) // UNROLL, step, 0)


def couple_kernel(pairs, per, table_ref, pair_ref, slot_ref, weight_ref, used_ref, s_ref, *refs):
    count = table_ref.shape[1]
    shards = refs[:count]
    keep_out, send_out, held, cat, acc, sem = refs[count:]
    me = lax.axis_index("pair")
    occ = lax.axis_index("occ")
    occs = pairs // per
    copies = []
    for k in range(count):
        at = table_ref[me, k] * per
        copies.append(pltpu.make_async_copy(shards[k], held.at[pl.ds(at, per)], sem.at[k]))
    for c in copies:
        c.start()
    acc[...] = jnp.zeros_like(acc)
    width = held.shape[-1]
    for c in copies:
        c.wait()

    def halve(t, carry):
        high, low = split(held[t])
        cat[t, :width, :width] = high
        cat[t, width:, :width] = high
        cat[t, :width, width:] = low
        cat[t, width:, width:] = jnp.zeros_like(low)
        return carry

    lax.fori_loop(0, held.shape[0], halve, 0)

    def step(g, carry):
        for k in range(UNROLL):
            i = g * UNROLL + k
            p = pair_ref[i]
            both = s_ref[i]
            inner = jnp.dot(both, cat[slot_ref[i]], preferred_element_type=F32)
            inner = (inner[:, :width] + inner[:, width:]) * weight_ref[i]
            ih, il = split(inner)
            sh, sl = both[:, :width], both[:, width:]
            lhs = jnp.concatenate([ih, il], axis=1)
            rhs = jnp.concatenate(
                [
                    jnp.concatenate([sh, sh], axis=1),
                    jnp.concatenate([sl, jnp.zeros_like(sl)], axis=1),
                ],
                axis=0,
            )
            outer = lax.dot_general(
                lhs, rhs, (((1,), (1,)), ((), ())), preferred_element_type=F32
            )
            acc[p] += outer[:, :width] + outer[:, width:]
        return carry

    lax.fori_loop(0, (used_ref[0] + UNROLL - 1) // UNROLL, step, 0)
    half = occs // 2
    for away in range(half):
        chip = lax.rem(occ // 2 + away, half)
        core = lax.rem(occ, 2)
        keep_out[away] = acc[pl.ds((chip * 2 + core) * per, per)]
        send_out[away] = acc[pl.ds((chip * 2 + 1 - core) * per, per)]


def spec(space):
    return pl.BlockSpec(memory_space=space)


def local(
    order,
    amplitudes,
    exchange_ints,
    pno_energy,
    pair_shift,
    coefficients,
    domain_tiles,
    couple_owner,
    couple_index,
    couple_weight,
):
    pairs, width = amplitudes.shape[:2]
    domain = coefficients.shape[1]
    tiles = domain_tiles.shape[1]
    size = domain // tiles
    per_pair = couple_index.shape[2]
    count = lax.axis_size("pair")
    occs = lax.axis_size("occ")
    half = occs // 2
    per = pairs // occs
    occ = lax.axis_index("occ")
    total = occs * pairs * per_pair
    couples = occs * per_pair
    shape = jax.ShapeDtypeStruct
    table = jnp.asarray(ring_table(order))

    blocks = coefficients.reshape(pairs, tiles, size, width)
    own_coef, own_amp = pl.pallas_call(
        functools.partial(prep_kernel, per),
        out_shape=(shape((per, tiles, size, width), BF16), shape((per, width, width), F32)),
        in_specs=[spec(SMEM), spec(pl.ANY), spec(pl.ANY)],
        out_specs=(spec(VMEM), spec(VMEM)),
        scratch_shapes=[pltpu.SemaphoreType.DMA((per * tiles + 1,))],
        compiler_params=pltpu.CompilerParams(vmem_limit_bytes=8 << 20),
        name="prep",
    )(domain_tiles, blocks, amplitudes)
    own_coef = own_coef.reshape(per, domain, width)
    coef_held = ring_gather(order, own_coef)
    amp_held = ring_gather(order, own_amp)

    turned = pl.pallas_call(
        turn_kernel,
        out_shape=shape((pairs, width, domain), BF16),
        in_specs=[spec(SMEM), spec(VMEM)],
        out_specs=spec(VMEM),
        compiler_params=pltpu.CompilerParams(vmem_limit_bytes=8 << 20),
        name="turn",
    )(domain_tiles, blocks)

    partner = (couple_owner[..., 0] * pairs + couple_index).astype(F32)
    mine = jnp.stack([partner[0], couple_weight[0]])
    every = lax.all_gather(mine, "occ")
    every = jnp.transpose(every, (1, 2, 0, 3)).reshape(2, total)
    partner = every[0].astype(jnp.int32)
    place = partner % pairs - occ * per
    slots = jnp.where((place >= 0) & (place < per), partner // pairs * per + place, -1)
    room = total + UNROLL

    s_both, pair_list, slot_list, weight_list, used = pl.pallas_call(
        functools.partial(overlap_kernel, couples),
        out_shape=(
            shape((room, width, 2 * width), BF16),
            shape((room,), jnp.int32),
            shape((room,), jnp.int32),
            shape((room,), F32),
            shape((1,), jnp.int32),
        ),
        in_specs=[spec(SMEM)] * 3 + [spec(VMEM)] + [spec(pl.ANY)] * count,
        out_specs=(spec(VMEM),) + (spec(SMEM),) * 4,
        scratch_shapes=[
            VMEM((count * per, domain, width), BF16),
            pltpu.SemaphoreType.DMA((count,)),
        ],
        compiler_params=pltpu.CompilerParams(vmem_limit_bytes=48 << 20),
        name="overlap",
    )(table, slots, every[1], turned, *coef_held)

    def coupled(held):
        return pl.pallas_call(
            functools.partial(couple_kernel, pairs, per),
            out_shape=(shape((half, per, width, width), F32),) * 2,
            in_specs=[spec(SMEM)] * 5 + [spec(VMEM)] + [spec(pl.ANY)] * count,
            out_specs=(spec(VMEM),) * 2,
            scratch_shapes=[
                VMEM((count * per, width, width), F32),
                VMEM((count * per, 2 * width, 2 * width), BF16),
                VMEM((pairs, width, width), F32),
                pltpu.SemaphoreType.DMA((count,)),
            ],
            compiler_params=pltpu.CompilerParams(vmem_limit_bytes=52 << 20),
            name="couple",
        )(table, pair_list, slot_list, weight_list, used, s_both, *held)

    core_swap = [(o, o ^ 1) for o in range(occs)]

    def chip_shift(value, away):
        return lax.ppermute(
            value, "occ", [(o, (o + 2 * away) % occs) for o in range(occs)]
        )

    def quarter(value, first):
        return lax.dynamic_slice_in_dim(value, first * per, per, 0)

    def spread(energy, shift):
        return energy[:, :, None] + energy[:, None, :] + shift[:, None, None]

    def column(value):
        return jnp.stack([quarter(value, (occ + 2 * a) % occs) for a in range(half)])

    keep, send = coupled(amp_held)
    summed = keep + lax.ppermute(send, "occ", core_swap)
    part = summed[0]
    for away in range(1, half):
        part = part + chip_shift(summed[away], away)
    denominator = spread(quarter(pno_energy, occ), quarter(pair_shift, occ))
    residual = quarter(exchange_ints, occ) + denominator * own_amp - part
    current = own_amp - residual / denominator

    keep, send = coupled(ring_gather(order, current))
    summed = keep + lax.ppermute(send, "occ", core_swap)
    totals = summed
    for away in range(1, half):
        moved = chip_shift(summed, away)
        totals = totals + jnp.roll(moved, -away, axis=0)
    currents = jnp.stack(
        [current] + [chip_shift(current, half - away) for away in range(1, half)]
    )
    energies = column(pno_energy)
    shifts = column(pair_shift)
    denominators = (
        energies[:, :, :, None] + energies[:, :, None, :] + shifts[:, :, None, None]
    )
    residuals = column(exchange_ints) + denominators * currents - totals
    updates = currents - residuals / denominators
    mine = jnp.stack([updates, residuals])
    other = lax.ppermute(mine, "occ", core_swap)
    core = occ % 2
    even = jnp.where(core == 0, mine, other)
    odd = jnp.where(core == 0, other, mine)
    both = jnp.stack([even, odd], axis=2)
    both = jnp.roll(both, occ // 2, axis=1).reshape(2, pairs, width, width)
    return both[0], both[1]


def solution(mesh):
    in_specs = (
        P("pair", None, None),
        P("pair", None, None),
        P("pair", None),
        P("pair"),
        P("pair", None, None),
        P("pair", None),
        P("occ", "pair", None, None),
        P("occ", "pair", None),
        P("occ", "pair", None),
    )
    out_specs = (P("pair", None, None), P("pair", None, None))
    return jax.shard_map(
        functools.partial(local, ring_order(mesh)),
        mesh=mesh,
        in_specs=in_specs,
        out_specs=out_specs,
        check_vma=False,
    )
```
